256 devices in a mesh: groups: 2 (over y), blk: 16 (over z), ulysses: 4 (over x), cfg: 2 (over core).
Axes of the slice: x: 4, y: 2, z: 16, core: 2. Of those that a mesh axis runs over, the one named last changes fastest.
The devices are a block of a 4x16x16 slice.
Arguments:
- img_tokens: bfloat16 [2, 2, 4096, 2432], P('cfg', 'groups', ('blk', 'ulysses')), parts along dimension 1, may hold values from -72 to 72
- text_tokens: bfloat16 [2, 2, 384, 2432], P('cfg', 'groups', ('blk', 'ulysses')), parts along dimension 1, may hold values from -6 to 6
- text_lengths: int32 [2, 2], P('cfg', 'groups'), parts along dimension 1, may hold values from 96 to 384
- timestep: int32 [2], P('groups'), parts along dimension 0, may hold values from 0 to 999
- pooled: float32 [2, 2, 2432], P(None, 'groups'), parts along dimension 1, may hold values from -6 to 6
- time_weight: bfloat16 [256, 2432], replicated, may hold values from -0.375 to 0.375
- time_second: bfloat16 [2432, 2432], P(None, ('blk', 'ulysses', 'cfg')), may hold values from -0.125 to 0.125
- mod_weight: bfloat16 [2432, 24320], P(None, ('blk', 'ulysses', 'cfg')), may hold values from -0.125 to 0.125
- proj_weight: bfloat16 [5, 2432, 2048], P(None, None, ('ulysses', 'cfg')), may hold values from -0.125 to 0.125
- out_weight: bfloat16 [2048, 2432], P(('ulysses', 'cfg')), may hold values from -0.125 to 0.125
- expand_weight: bfloat16 [2432, 7168], P('blk', ('ulysses', 'cfg')), may hold values from -0.125 to 0.125
- reduce_weight: bfloat16 [7168, 2432], P(('ulysses', 'cfg'), 'blk'), may hold values from -0.0625 to 0.0625
- qk_gain: float32 [3, 64], replicated, may hold values from 0.5 to 10
- final_weight: bfloat16 [2432, 64], replicated, may hold values from -0.125 to 0.125
Outputs:
- guided: float32 [2, 16, 128, 128], P('groups', None, ('blk', 'ulysses', 'cfg')), parts along dimension 0
The draws below stay inside these ranges and needn't reach their ends.
There are 2 independent parts, one for each index of `groups`. The reference program is written for one: setup_inputs(seed, part) draws one part's arguments, and reference() takes and returns one part's arrays. A program takes and returns all parts, laid end to end along the dimension named above; an argument that names none is the same for every part. Nothing has to cross between parts.
All inputs are finite; a program needn't handle non-finite values.
Results may differ from the reference program's by a relative error of at most 0.011.
The reference program's roundings to bfloat16 on the way count: a program that leaves them out, or rounds other values in their place, can miss the bound.
Values may be sent and summed in bfloat16 or wider, within the bound.
A program may use at most 192 MiB of HBM per device.

```python
import math
import jax
import jax.numpy as jnp
from jax import lax

D = 2432
HEADS = 32
HD = 64
LAT = 16
FREQ = 256
FF = 7168
PROMPTS = 1
IMG_DEV = 64
INNER = 2048
PATCH_OUT = 64
IMG = 4096
TXT = 384
N_ULYSSES = 4
N_CFG = 2


def draw_img_tokens(key, part):
    base_key, row_key, col_key = jax.random.split(jax.random.fold_in(key, 11), 3)
    full_shape = (2, PROMPTS, IMG, D)
    base_draw = jnp.clip(jax.random.normal(base_key, full_shape, jnp.float32), -4.0, 4.0)
    row_top = math.log(4.0)
    row_scale = jnp.exp(jax.random.uniform(row_key, (2, PROMPTS, IMG, 1), jnp.float32, 0.0, row_top))
    col_scale = jnp.exp(jax.random.uniform(col_key, (1, 1, 1, D), jnp.float32, math.log(0.5), math.log(2.0)))
    return (base_draw * row_scale * col_scale).astype(jnp.bfloat16)


def draw_qk_gain(key, part):
    gain_key = jax.random.fold_in(key, 23)
    low_end = math.log(0.5)
    high_end = math.log(2.0)
    return jnp.exp(jax.random.uniform(gain_key, (3, HD), jnp.float32, low_end, high_end))


def shard_levels(key, shape, cuts, smallest, largest):
    def one(position, blocks):
        heights = jax.random.uniform(jax.random.fold_in(jax.random.fold_in(key, 6), position), (blocks,), jnp.float32, smallest / len(cuts), largest / len(cuts))
        return jnp.repeat(jnp.exp(heights), shape[position] // blocks).reshape((-1,) + (1,) * (len(shape) - position - 1))

    level = one(*cuts[0])
    for cut in cuts[1:]:
        level = level * one(*cut)
    return level


def normal_values(stream_key, dims, deviation, bound, shards=(), kind=jnp.bfloat16):
    factor_of = shard_levels(stream_key, dims, shards, -0.22, 0.18) if shards else 1.0
    result = jax.random.normal(stream_key, dims, jnp.float32) * deviation * factor_of
    return jnp.minimum(jnp.maximum(result, -bound), bound).astype(kind)


def setup_inputs(seed: int = 0, part: int = 0) -> dict:
    key_list = jax.random.split(jax.random.key(seed), 15)
    part_keys = jax.random.split(jax.random.fold_in(key_list[14], part), 15)
    img_tokens = draw_img_tokens(jax.random.fold_in(jax.random.fold_in(key_list[14], part), 71), part)
    text_tokens = normal_values(part_keys[1], (2, PROMPTS, TXT, D), 1.0, 6.0, ((0, 2), (2, 64)))
    text_lengths = jax.random.randint(part_keys[2], (2, PROMPTS), TXT // 4, TXT + 1).astype(jnp.int32)
    timestep = jax.random.randint(part_keys[3], (PROMPTS,), 0, 1000).astype(jnp.int32)
    pooled = normal_values(part_keys[4], (2, PROMPTS, D), 1.0, 6.0, (), jnp.float32)
    time_weight = normal_values(key_list[5], (FREQ, D), FREQ ** -0.5, 0.375)
    time_second = normal_values(key_list[6], (D, D), D ** -0.5, 0.125, ((1, 128),))
    mod_weight = normal_values(key_list[7], (D, 10 * D), D ** -0.5, 0.125, ((1, 128),))
    proj_weight = normal_values(key_list[8], (5, D, INNER), D ** -0.5, 0.125, ((2, 8),))
    out_weight = normal_values(key_list[9], (INNER, D), INNER ** -0.5, 0.125, ((0, 8),))
    expand_weight = normal_values(key_list[10], (D, FF), D ** -0.5, 0.125, ((0, 16), (1, 8)))
    reduce_weight = normal_values(key_list[11], (FF, D), FF ** -0.5, 0.0625, ((0, 8), (1, 16)))
    qk_gain = draw_qk_gain(jax.random.fold_in(key_list[14], 71), part)
    final_weight = normal_values(key_list[13], (D, PATCH_OUT), D ** -0.5, 0.125)
    return {"img_tokens": img_tokens, "text_tokens": text_tokens, "text_lengths": text_lengths, "timestep": timestep, "pooled": pooled, "time_weight": time_weight, "time_second": time_second, "mod_weight": mod_weight, "proj_weight": proj_weight, "out_weight": out_weight, "expand_weight": expand_weight, "reduce_weight": reduce_weight, "qk_gain": qk_gain, "final_weight": final_weight}


GUIDANCE = 3.5
LN_EPS = 1e-06
RMS_EPS = 1e-06
NEG_FILL = -1e+30

def sinusoid(timestep, feature_count):
    half_width = feature_count // 2
    frequency = jnp.exp(-math.log(10000.0) * jnp.arange(half_width, dtype=jnp.float32) / half_width)
    angles = timestep.astype(jnp.float32)[:, None] * frequency[None, :]
    return jnp.concatenate([jnp.cos(angles), jnp.sin(angles)], axis=1)

def layer_norm(values):
    average = lax.optimization_barrier(jnp.mean(values, axis=-1, keepdims=True))
    centred = values - average
    variance = lax.optimization_barrier(jnp.mean(centred * centred, axis=-1, keepdims=True))
    return centred * lax.rsqrt(variance + LN_EPS)

def modulate(values, shift, scale):
    return (layer_norm(values.astype(jnp.float32)) * (1.0 + scale) + shift).astype(jnp.bfloat16)

def rms_heads(values, gain):
    head_size = gain.shape[0]
    shaped = values.reshape(values.shape[:-1] + (values.shape[-1] // head_size, head_size))
    inverse = lax.rsqrt(lax.optimization_barrier(jnp.mean(shaped * shaped, axis=-1, keepdims=True)) + RMS_EPS)
    return (shaped * inverse * gain).reshape(values.shape).astype(jnp.bfloat16)

def finish(img_proj, txt_proj, gain_rows):
    img_set = jnp.stack([rms_heads(img_proj[0], gain_rows[0]), rms_heads(img_proj[1], gain_rows[1]), img_proj[2].astype(jnp.bfloat16)])
    txt_set = jnp.stack([rms_heads(txt_proj[0], gain_rows[2]), txt_proj[1].astype(jnp.bfloat16)])
    return (img_set, txt_set)

def head_attention(query_head, key_head, value_head, usable):
    scores = jnp.dot(query_head, key_head.T, preferred_element_type=jnp.float32) * (1.0 / math.sqrt(query_head.shape[1]))
    scores = jnp.where(usable[None, :], scores, NEG_FILL)
    row_max = lax.optimization_barrier(jnp.max(scores, axis=1, keepdims=True))
    weights = jnp.where(usable[None, :], jnp.exp(scores - row_max), 0.0)
    row_total = lax.optimization_barrier(jnp.sum(weights, axis=1, keepdims=True))
    mixed = jnp.dot(weights.astype(jnp.bfloat16), value_head, preferred_element_type=jnp.float32) / row_total
    return mixed.astype(jnp.bfloat16)

def feed_forward(feed_input, expand_weight, reduce_weight):
    feed_hidden = jax.nn.gelu(jnp.dot(feed_input, expand_weight, preferred_element_type=jnp.float32), approximate=True).astype(jnp.bfloat16)
    group_count = N_ULYSSES * N_CFG
    group_width = reduce_weight.shape[0] // group_count
    feed_out = jnp.zeros((feed_input.shape[0], reduce_weight.shape[1]), jnp.float32)
    for group in range(group_count):
        term = jnp.dot(feed_hidden[:, group * group_width:(group + 1) * group_width], reduce_weight[group * group_width:(group + 1) * group_width], preferred_element_type=jnp.float32)
        term = lax.optimization_barrier(term.astype(jnp.bfloat16))
        feed_out = feed_out + term.astype(jnp.float32)
    return feed_out

def one_branch(image_rows, text_rows, length, mod_rows, proj_weight, out_weight, expand_weight, reduce_weight, qk_gain, final_weight):
    h_img = modulate(image_rows, mod_rows[0], mod_rows[1])
    h_txt = modulate(text_rows, mod_rows[4], mod_rows[3])
    img_proj = jnp.stack([jnp.dot(h_img, proj_weight[j], preferred_element_type=jnp.float32) for j in range(3)])
    txt_proj = jnp.stack([jnp.dot(h_txt, proj_weight[j], preferred_element_type=jnp.float32) for j in (3, 4)])
    img_set, txt_set = finish(img_proj, txt_proj, qk_gain)
    key_rows = jnp.concatenate([img_set[1], txt_set[0]], axis=0)
    value_rows = jnp.concatenate([img_set[2], txt_set[1]], axis=0)
    usable = jnp.concatenate([jnp.ones((IMG,), dtype=bool), jnp.arange(TXT, dtype=jnp.int32) < length])
    query_stack = img_set[0].reshape(IMG, HEADS, HD).transpose(1, 0, 2)
    key_stack = key_rows.reshape(IMG + TXT, HEADS, HD).transpose(1, 0, 2)
    value_stack = value_rows.reshape(IMG + TXT, HEADS, HD).transpose(1, 0, 2)

    def per_head(triple):
        return head_attention(triple[0], triple[1], triple[2], usable)
    mixed = lax.map(per_head, (query_stack, key_stack, value_stack))
    mixed = mixed.transpose(1, 0, 2).reshape(IMG, INNER)
    grouped = mixed.reshape(IMG, N_ULYSSES, INNER // N_ULYSSES).astype(jnp.float32)
    weight_groups = out_weight.reshape(N_ULYSSES, INNER // N_ULYSSES, D).astype(jnp.float32)
    group_terms = jnp.einsum('igc,gcd->gid', grouped, weight_groups, precision=lax.Precision.HIGHEST)
    group_terms = lax.optimization_barrier(group_terms.astype(jnp.bfloat16))
    attended = lax.optimization_barrier(jnp.sum(group_terms.astype(jnp.float32), axis=0))
    residual = image_rows.astype(jnp.float32) + mod_rows[2] * attended
    feed_input = modulate(residual, mod_rows[7], mod_rows[8])
    feed_out = feed_forward(feed_input, expand_weight, reduce_weight)
    second_residual = residual + mod_rows[9] * feed_out
    final_rows = modulate(second_residual, mod_rows[6], mod_rows[5])
    noise = jnp.dot(final_rows, final_weight, preferred_element_type=jnp.float32)
    noise = noise.reshape(IMG // IMG_DEV, IMG_DEV, 2, 2, LAT).transpose(4, 0, 2, 1, 3)
    return noise.reshape(LAT, 2 * IMG // IMG_DEV, 2 * IMG_DEV)

def reference(img_tokens, text_tokens, text_lengths, timestep, pooled, time_weight, time_second, mod_weight, proj_weight, out_weight, expand_weight, reduce_weight, qk_gain, final_weight):
    sinusoid_rows = sinusoid(timestep, time_weight.shape[0]).astype(jnp.bfloat16)
    time_hidden = jax.nn.silu(jnp.dot(sinusoid_rows, time_weight, preferred_element_type=jnp.float32)).astype(jnp.bfloat16)
    time_embed = jnp.dot(time_hidden, time_second, preferred_element_type=jnp.float32)
    acted = jax.nn.silu(time_embed[None] + pooled).astype(jnp.bfloat16)
    modulation = jnp.dot(acted.reshape(2 * PROMPTS, D), mod_weight, preferred_element_type=jnp.float32)
    modulation = modulation.reshape(2, PROMPTS, 10, D)
    results = []
    for prompt in range(PROMPTS):
        noises = []
        for branch in range(2):
            noises.append(one_branch(img_tokens[branch, prompt], text_tokens[branch, prompt], text_lengths[branch, prompt], modulation[branch, prompt], proj_weight, out_weight, expand_weight, reduce_weight, qk_gain, final_weight))
        noise_cond = noises[0]
        noise_uncond = noises[1]
        results.append(noise_uncond + GUIDANCE * (noise_cond - noise_uncond))
    return jnp.stack(results)
```

```python
import functools
import math

import jax
import jax.numpy as jnp
from jax import lax
from jax.experimental import pallas as pl
from jax.experimental.pallas import tpu as pltpu
from jax.sharding import PartitionSpec as P

GUIDANCE = 3.5
LN_EPS = 1e-06
RMS_EPS = 1e-06
NEG_FILL = -1e30
MESH = pl.DeviceIdType.MESH
VMEM = pltpu.VMEM
BF16 = jnp.bfloat16
F32 = jnp.float32
VMEM_LIMIT = 60 * 1024 * 1024


def place():
    return lax.axis_index("blk"), lax.axis_index("ulysses"), lax.axis_index("cfg")


class Wires:
    def __init__(self, send_sems, recv_sems):
        self.send_sems, self.recv_sems, self.count, self.sent = (send_sems, recv_sems, 0, [])

    def send(self, src, dst, **device):
        number = self.count
        self.count += 1
        copy = pltpu.make_async_remote_copy(
            src_ref=src,
            dst_ref=dst,
            send_sem=self.send_sems.at[number],
            recv_sem=self.recv_sems.at[number],
            device_id=device,
            device_id_type=MESH,
        )
        copy.start()
        self.sent.append(copy)
        return number

    def arrive(self, number, dst, **device):
        pltpu.make_async_remote_copy(
            src_ref=dst,
            dst_ref=dst,
            send_sem=self.send_sems.at[number],
            recv_sem=self.recv_sems.at[number],
            device_id=device,
            device_id_type=MESH,
        ).wait_recv()

    def drain(self):
        for copy in self.sent:
            copy.wait_send()
        self.sent = []


def greet(devices):
    barrier = pltpu.get_barrier_semaphore()
    for device in devices:
        pl.semaphore_signal(barrier, inc=1, device_id=device, device_id_type=MESH)
    pl.semaphore_wait(barrier, len(devices))


def ring_greetings(u, c, nu):
    return [
        {"ulysses": lax.rem(u + 1, nu)},
        {"ulysses": lax.rem(u + nu - 1, nu)},
        {"cfg": 1 - c},
    ]


def sinusoid(timestep, feature_count):
    half_width = feature_count // 2
    frequency = jnp.exp(-math.log(10000.0) * jnp.arange(half_width, dtype=F32) / half_width)
    angles = timestep.astype(F32)[:, None] * frequency[None, :]
    return jnp.concatenate([jnp.cos(angles), jnp.sin(angles)], axis=1)


def normalized(values, shift, scale):
    average = jnp.mean(values, axis=-1, keepdims=True)
    centred = values - average
    variance = jnp.mean(centred * centred, axis=-1, keepdims=True)
    return centred * lax.rsqrt(variance + LN_EPS) * (1.0 + scale) + shift


def spread_kernel(nb, nu, own_branch, part_ref, out_ref, buf, send1, recv1, send2, recv2, local_sem):
    b, u, c = place()
    per = 2 * nu
    me = u * 2 + c
    greet(
        [{"ulysses": lax.rem(me + k, per) // 2, "cfg": lax.rem(me + k, per) % 2} for k in range(1, per)]
        + [{"blk": lax.rem(b + k, nb)} for k in range(1, nb)]
    )
    near, far = (Wires(send1, recv1), Wires(send2, recv2))
    own = pltpu.make_async_copy(part_ref.at[c if own_branch else 0], buf.at[b, me], local_sem)
    own.start()
    for k in range(1, per):
        peer = lax.rem(me + k, per)
        near.send(
            part_ref.at[peer % 2 if own_branch else 0],
            buf.at[b, me],
            ulysses=peer // 2,
            cfg=peer % 2,
        )
    own.wait()
    for k in range(1, per):
        peer = lax.rem(me + per - k, per)
        near.arrive(k - 1, buf.at[b, peer], ulysses=peer // 2, cfg=peer % 2)
    for k in range(1, nb):
        far.send(buf.at[b], buf.at[b], blk=lax.rem(b + k, nb))
    for k in range(1, nb):
        peer = lax.rem(b + nb - k, nb)
        far.arrive(k - 1, buf.at[peer], blk=peer)
    near.drain()
    far.drain()
    out_ref[...] = buf[...]


def spread(mesh, part, own_branch, call_id):
    nb, nu = (mesh.shape["blk"], mesh.shape["ulysses"])
    width = part.shape[2]
    return pl.pallas_call(
        functools.partial(spread_kernel, nb, nu, own_branch),
        out_shape=jax.ShapeDtypeStruct((nb, 2 * nu, 1, width), F32),
        in_specs=[pl.BlockSpec(memory_space=VMEM)],
        out_specs=pl.BlockSpec(memory_space=VMEM),
        scratch_shapes=[
            VMEM((nb, 2 * nu, 1, width), F32),
            pltpu.SemaphoreType.DMA((2 * nu,)),
            pltpu.SemaphoreType.DMA((2 * nu,)),
            pltpu.SemaphoreType.DMA((nb,)),
            pltpu.SemaphoreType.DMA((nb,)),
            pltpu.SemaphoreType.DMA,
        ],
        compiler_params=pltpu.CompilerParams(collective_id=call_id, has_side_effects=True),
        name=f"spread_{call_id}",
    )(part)


def ring_share(wires, first, second, u, c, nu):
    right, left, opposite = (lax.rem(u + 1, nu), lax.rem(u + nu - 1, nu), lax.rem(u + 2, nu))
    slot = lambda uu, cc: cc * nu + uu
    mine, other = (slot(u, c), 1 - c)
    across = {}

    def push(view, where, **device):
        return wires.send(view(where), view(where), **device)

    go_right, go_left = ({}, {})
    for view in first + second:
        go_right[view] = push(view, mine, ulysses=right)
    for view in second + first:
        go_left[view] = push(view, mine, ulysses=left)
    for view in first + second:
        across[view, "mine"] = push(view, mine, cfg=other)
    on_right, on_left = ({}, {})
    for k in range(len(first + second)):
        for views, got, came, onward, far in (
            (first + second, go_right, left, on_right, first),
            (second + first, go_left, right, on_left, second),
        ):
            if k >= len(views):
                continue
            view = views[k]
            wires.arrive(got[view], view(slot(came, c)), ulysses=came)
            if view in far:
                onward[view] = push(view, slot(came, c), ulysses=right if got is go_right else left)
            across[view, "left" if got is go_right else "right"] = push(view, slot(came, c), cfg=other)
    for view in first + second:
        forward, came = (on_right, left) if view in first else (on_left, right)
        wires.arrive(forward[view], view(slot(opposite, c)), ulysses=came)
        across[view, "opposite"] = push(view, slot(opposite, c), cfg=other)
    for (view, source), number in across.items():
        uu = {"mine": u, "left": left, "right": right, "opposite": opposite}[source]
        wires.arrive(number, view(slot(uu, other)), cfg=other)


def project_kernel(nu, img_ref, txt_ref, mod_ref, gain_ref, w_ref, out_ref, himg, htxt, w_buf, stage, send, recv, local):
    b, u, c = place()
    rows, depth = img_ref.shape
    text_rows = txt_ref.shape[0]
    load = pltpu.make_async_copy(w_ref, w_buf, local)
    load.start()
    mine = c * nu + u
    half = rows // 2
    for part in range(2):
        span = pl.ds(part * half, half)
        himg[mine, span] = normalized(
            img_ref[span].astype(F32), mod_ref[0:1], mod_ref[1:2]
        ).astype(BF16)
    htxt[...] = jnp.zeros_like(htxt)
    htxt[mine, 0:text_rows] = normalized(
        txt_ref[...].astype(F32), mod_ref[4:5], mod_ref[3:4]
    ).astype(BF16)
    greet(ring_greetings(u, c, nu))
    wires = Wires(send, recv)
    ring_share(
        wires,
        [lambda s: himg.at[s, pl.ds(0, half)], lambda s: htxt.at[s, pl.ds(0, 8)]],
        [lambda s: himg.at[s, pl.ds(half, half)]],
        u,
        c,
        nu,
    )
    load.wait()
    width = w_buf.shape[2]
    heads = width // 64
    lane = lax.broadcasted_iota(jnp.int32, (width, width), 0) // 64
    group = jnp.where(lane == lax.broadcasted_iota(jnp.int32, (width, width), 1) // 64, 1.0 / 64, 0.0)

    def unit(values, gain):
        square = values * values
        high = square.astype(BF16)
        low = (square - high.astype(F32)).astype(BF16)
        ones = group.astype(BF16)
        mean = jnp.dot(high, ones, preferred_element_type=F32) + jnp.dot(
            low, ones, preferred_element_type=F32
        )
        return values * lax.rsqrt(mean + RMS_EPS) * gain

    img_span = nu * rows
    for branch in range(2):
        x = himg[pl.ds(branch * nu, nu)].reshape(img_span, depth)
        q = unit(jnp.dot(x, w_buf[0], preferred_element_type=F32), gain_ref[0:1]) * 0.125
        q = q.astype(BF16).astype(F32)
        for h in range(heads):
            pair, odd = (h // 2, h % 2)
            block = q[:, pair * 128 : pair * 128 + 128]
            turned = pltpu.roll(block, 64, 1)
            low, high = (turned, block) if odd else (block, turned)
            lanes = lax.broadcasted_iota(jnp.int32, (img_span // 2, 128), 1)
            out_ref[branch * heads + h, pl.ds(img_span + 32, img_span // 2)] = jnp.where(
                lanes < 64, low[: img_span // 2], high[img_span // 2 :]
            ).astype(BF16)
        k = unit(jnp.dot(x, w_buf[1], preferred_element_type=F32), gain_ref[1:2])
        v = jnp.dot(x, w_buf[2], preferred_element_type=F32)
        t = htxt[pl.ds(branch * nu, nu)].reshape(nu * 16, depth)
        tk = unit(jnp.dot(t, w_buf[3], preferred_element_type=F32), gain_ref[2:3])
        tv = jnp.dot(t, w_buf[4], preferred_element_type=F32)
        for keys, values, at, live in ((k, v, 0, None), (tk, tv, img_span, 8)):
            for h in range(heads):
                pair, odd = (h // 2, h % 2)
                kb = keys[:, pair * 128 : pair * 128 + 128]
                vb = values[:, pair * 128 : pair * 128 + 128]
                kb = pltpu.roll(kb, 64, 1) if odd else kb
                vb = vb if odd else pltpu.roll(vb, 64, 1)
                lanes = lax.broadcasted_iota(jnp.int32, kb.shape, 1)
                both = jnp.where(lanes < 64, kb, vb)
                if live is not None:
                    both = jnp.concatenate([both[i * 16 : i * 16 + live] for i in range(nu)], axis=0)
                out_ref[branch * heads + h, pl.ds(at, both.shape[0])] = both.astype(BF16)
    wires.drain()


def project(mesh, img, txt, mod, gain, weights):
    nu = mesh.shape["ulysses"]
    rows, depth = img.shape
    width = weights.shape[2]
    units = 2 * (width // 64)
    vm = pl.BlockSpec(memory_space=VMEM)
    return pl.pallas_call(
        functools.partial(project_kernel, nu),
        out_shape=jax.ShapeDtypeStruct((units, nu * rows + 32 + nu * rows // 2, 128), BF16),
        in_specs=[vm, vm, vm, vm, pl.BlockSpec(memory_space=pl.ANY)],
        out_specs=vm,
        scratch_shapes=[
            VMEM((2 * nu, rows, depth), BF16),
            VMEM((2 * nu, 16, depth), BF16),
            VMEM(weights.shape, BF16),
            VMEM((8, 128), F32),
            pltpu.SemaphoreType.DMA((32,)),
            pltpu.SemaphoreType.DMA((32,)),
            pltpu.SemaphoreType.DMA,
        ],
        compiler_params=pltpu.CompilerParams(
            collective_id=2, has_side_effects=True, vmem_limit_bytes=VMEM_LIMIT
        ),
        name="project",
    )(img, txt, mod, gain, weights)


def attend_kernel(
    nb, nu, unit_ref, bias_ref, wo_ref, out_ref,
    kvb, qb, k_t, kv1, scores, stage, heads_in, wo, mixed,
    kv_send, kv_recv, q_send, q_recv, f_send, f_recv, o_send, o_recv, w_send, w_recv, local, local_w,
):
    b, u, c = place()
    other = 1 - c
    side = lax.rem(b, 2)
    units = unit_ref.shape[0]
    kv_rows = kvb.shape[1]
    img_span = kv_rows - 32
    q_rows = qb.shape[1]
    tiles = qb.shape[0]
    branch = b // (nb // 2)
    peers = [{"blk": lax.rem(b + k, nb), "cfg": cc} for k in range(1, nb) for cc in range(2)]
    load_w = pltpu.make_async_copy(wo_ref, wo.at[c], local_w)
    load_w.start()
    greet(peers + [{"cfg": other}])

    def kv_copy(i, blk, core, src):
        return pltpu.make_async_remote_copy(
            src_ref=src, dst_ref=kvb.at[b], send_sem=kv_send.at[i], recv_sem=kv_recv.at[b // 2],
            device_id={"blk": blk, "cfg": core}, device_id_type=MESH,
        )

    def q_copy(i, blk, core, src):
        return pltpu.make_async_remote_copy(
            src_ref=src, dst_ref=qb.at[b // 2], send_sem=q_send.at[i], recv_sem=q_recv.at[b // 2],
            device_id={"blk": blk, "cfg": core}, device_id_type=MESH,
        )

    def local_kv(i):
        return pltpu.make_async_copy(unit_ref.at[i, pl.ds(0, kv_rows)], kvb.at[2 * i + c], local.at[0])

    def local_q(i):
        return pltpu.make_async_copy(unit_ref.at[i, pl.ds(kv_rows, q_rows)], qb.at[i], local.at[1])

    for i in range(units):
        blk = 2 * i + c

        @pl.when(blk != b)
        def _():
            kv_copy(i, blk, side, unit_ref.at[i, pl.ds(0, kv_rows)]).start()
            q_copy(i, blk, side, unit_ref.at[i, pl.ds(kv_rows, q_rows)]).start()

        @pl.when(blk == b)
        def _():
            local_kv(i).start()
            local_q(i).start()

    load_w.wait()
    share_w = pltpu.make_async_remote_copy(
        src_ref=wo.at[c], dst_ref=wo.at[c], send_sem=w_send, recv_sem=w_recv,
        device_id={"cfg": other}, device_id_type=MESH,
    )
    share_w.start()

    def arrival(ref, sem, blk):
        return pltpu.make_async_remote_copy(
            src_ref=ref, dst_ref=ref, send_sem=kv_send.at[0], recv_sem=sem,
            device_id={"blk": blk, "cfg": side}, device_id_type=MESH,
        )

    def forward(i, blk):
        return pltpu.make_async_remote_copy(
            src_ref=kvb.at[blk], dst_ref=kvb.at[blk], send_sem=f_send.at[i], recv_sem=f_recv.at[i],
            device_id={"cfg": other}, device_id_type=MESH,
        )

    def prepare(blk):
        rows = kvb[blk]
        image = rows[:img_span]
        at = pl.multiple_of(blk * img_span, img_span)
        k_t[:, pl.ds(at, img_span)] = image.astype(F32).T.astype(BF16)
        lanes = lax.broadcasted_iota(jnp.int32, rows.shape, 1)
        ones = jnp.where(lanes < 64, jnp.ones_like(rows), rows)
        kv1[pl.ds(at, img_span)] = ones[:img_span]
        low = pl.multiple_of(nb * img_span + blk * 32, 32)
        kv1[pl.ds(low, 32)] = ones[img_span:]

    for i in range(units):
        blk = 2 * i + c

        @pl.when(blk != b)
        def _():
            arrival(kvb.at[blk], kv_recv.at[i], blk).wait_recv()

        @pl.when(blk == b)
        def _():
            local_kv(i).wait()

        forward(i, blk).start()
        prepare(blk)
    for i in range(units):
        blk = 2 * i + other
        forward(i, blk).wait_recv()
        prepare(blk)
    text = jnp.concatenate([kvb[k, img_span:kv_rows] for k in range(nb)], axis=0)
    text_at = nb * img_span
    text_keys = nb * 32
    k_t[:, text_at : text_at + text_keys] = text.astype(F32).T.astype(BF16)
    for i in range(units):
        blk = 2 * i + c

        @pl.when(blk != b)
        def _():
            arrival(qb.at[i], q_recv.at[i], blk).wait_recv()

        @pl.when(blk == b)
        def _():
            local_q(i).wait()

    key_count = text_at + text_keys
    step = 512
    lanes = lax.broadcasted_iota(jnp.int32, (q_rows, 128), 1)
    head = side * 4 + lax.rem(b // 2, 4)

    def o_copy(i, blk):
        return pltpu.make_async_remote_copy(
            src_ref=stage.at[i], dst_ref=heads_in.at[head], send_sem=o_send.at[i], recv_sem=o_recv.at[head],
            device_id={"blk": blk, "cfg": branch}, device_id_type=MESH,
        )

    def o_local(i):
        return pltpu.make_async_copy(stage.at[i], heads_in.at[head], local.at[0])

    @pl.loop(0, tiles)
    def _(i):
        packed = qb[i].astype(F32)
        low = jnp.where(lanes < 64, packed, 0.0)
        high = jnp.where(lanes < 64, pltpu.roll(packed, 64, 1), 0.0)
        q = jnp.concatenate([low, high], axis=0).astype(BF16)
        top = jnp.full((2 * q_rows, 128), NEG_FILL, F32)
        for at in range(0, key_count, step):
            block = jnp.dot(q, k_t[:, at : at + step], preferred_element_type=F32)
            if at >= text_at:
                block = block + bias_ref[branch, :, at - text_at : at - text_at + step]
            scores[:, at : at + step] = block
            for piece in range(0, step, 128):
                top = jnp.maximum(top, block[:, piece : piece + 128])
        row_max = jnp.max(top, axis=1, keepdims=True)
        total = jnp.zeros((2 * q_rows, 128), F32)
        for at in range(0, key_count, step):
            weights = jnp.exp(scores[:, at : at + step] - row_max).astype(BF16)
            total = total + jnp.dot(weights, kv1[at : at + step], preferred_element_type=F32)
        turned = pltpu.roll(total, 64, 1)
        first = turned[:q_rows] / total[:q_rows]
        second = total[q_rows:] / turned[q_rows:]
        stage[i] = jnp.where(lanes < 64, first, second).astype(BF16)
        blk = 2 * i + c
        mine = jnp.logical_and(blk == b, branch == c)

        @pl.when(mine)
        def _():
            o_local(i).start()

        @pl.when(jnp.logical_not(mine))
        def _():
            o_copy(i, blk).start()

    share_w.wait_recv()
    for h in range(8):
        source = (nb // 2) * c + 2 * (h % 4) + h // 4
        mine = jnp.logical_and(source == b, side == c)

        @pl.when(mine)
        def _():
            pltpu.make_async_copy(stage.at[0], heads_in.at[h], local.at[0]).wait()

        @pl.when(jnp.logical_not(mine))
        def _():
            pltpu.make_async_remote_copy(
                src_ref=heads_in.at[h], dst_ref=heads_in.at[h], send_sem=o_send.at[0], recv_sem=o_recv.at[h],
                device_id={"blk": source, "cfg": side}, device_id_type=MESH,
            ).wait_recv()

    for pair in range(4):
        even = heads_in[2 * pair].astype(F32)
        odd = heads_in[2 * pair + 1].astype(F32)
        span = slice(pair * 128, pair * 128 + 128)
        mixed[0:q_rows, span] = jnp.where(lanes < 64, even, pltpu.roll(odd, 64, 1)).astype(BF16)
        mixed[q_rows : 2 * q_rows, span] = jnp.where(lanes < 64, pltpu.roll(even, 64, 1), odd).astype(BF16)
    weight_rows = wo.shape[0] * wo.shape[1]
    out = jnp.dot(
        mixed[...], wo[...].reshape(weight_rows, wo.shape[2]), preferred_element_type=F32
    ).astype(BF16)
    out_ref[...] = out.reshape(out_ref.shape)
    share_w.wait_send()
    for i in range(units):
        blk = 2 * i + c

        @pl.when(blk != b)
        def _():
            kv_copy(i, blk, side, unit_ref.at[i, pl.ds(0, kv_rows)]).wait_send()
            q_copy(i, blk, side, unit_ref.at[i, pl.ds(kv_rows, q_rows)]).wait_send()

        forward(i, blk).wait_send()

        @pl.when(jnp.logical_not(jnp.logical_and(blk == b, branch == c)))
        def _():
            o_copy(i, blk).wait_send()


def attention(mesh, unit_rows, bias, out_weight, rows):
    nb, nu = (mesh.shape["blk"], mesh.shape["ulysses"])
    units = unit_rows.shape[0]
    img_span = nu * rows
    q_rows = img_span // 2
    kv_rows = img_span + 32
    keys = nb * kv_rows
    depth = out_weight.shape[1]
    dma = pltpu.SemaphoreType.DMA
    vm = pl.BlockSpec(memory_space=VMEM)
    return pl.pallas_call(
        functools.partial(attend_kernel, nb, nu),
        out_shape=jax.ShapeDtypeStruct((nu, rows, depth), BF16),
        in_specs=[vm, vm, pl.BlockSpec(memory_space=pl.ANY)],
        out_specs=vm,
        scratch_shapes=[
            VMEM((nb, kv_rows, 128), BF16),
            VMEM((units, q_rows, 128), BF16),
            VMEM((128, keys), BF16),
            VMEM((keys, 128), BF16),
            VMEM((2 * q_rows, keys), F32),
            VMEM((units, q_rows, 128), BF16),
            VMEM((8, q_rows, 128), BF16),
            VMEM((2, *out_weight.shape), BF16),
            VMEM((2 * q_rows, 512), BF16),
            dma((units,)), dma((units,)), dma((units,)), dma((units,)), dma((units,)), dma((units,)),
            dma((units,)), dma((8,)), dma, dma, dma((2,)), dma,
        ],
        compiler_params=pltpu.CompilerParams(
            collective_id=3, has_side_effects=True, vmem_limit_bytes=VMEM_LIMIT
        ),
        name="attend",
    )(unit_rows, bias, out_weight)


def ring_sum(wires, part, relay, staged, inbox, u, nu, emit):
    right, left, opposite = (lax.rem(u + 1, nu), lax.rem(u + nu - 1, nu), lax.rem(u + 2, nu))
    half = part.shape[1] // 2
    low, high = (pl.ds(0, half), pl.ds(half, half))
    far_r = wires.send(part.at[opposite, low], relay.at[0], ulysses=right)
    far_l = wires.send(part.at[opposite, high], relay.at[1], ulysses=left)
    near_r = wires.send(part.at[right, high], inbox.at[0, high], ulysses=right)
    near_l = wires.send(part.at[left, low], inbox.at[1, low], ulysses=left)
    wires.arrive(far_r, relay.at[0], ulysses=left)
    staged[0] = (part[right, low].astype(F32) + relay[0].astype(F32)).astype(BF16)
    last_r = wires.send(staged.at[0], inbox.at[0, low], ulysses=right)
    wires.arrive(far_l, relay.at[1], ulysses=right)
    staged[1] = (part[left, high].astype(F32) + relay[1].astype(F32)).astype(BF16)
    last_l = wires.send(staged.at[1], inbox.at[1, high], ulysses=left)
    wires.arrive(near_r, inbox.at[0, high], ulysses=left)
    wires.arrive(near_l, inbox.at[1, low], ulysses=right)
    wires.arrive(last_r, inbox.at[0, low], ulysses=left)
    wires.arrive(last_l, inbox.at[1, high], ulysses=right)

    @pl.loop(0, part.shape[1], step=16)
    def _(at):
        span = pl.ds(pl.multiple_of(at, 16), 16)
        total = part[u, span].astype(F32) + inbox[0, span].astype(F32) + inbox[1, span].astype(F32)
        emit(span, total)


def middle_kernel(nu, part, img_ref, mod_ref, all_ref, res_ref, relay, staged, inbox, feed, send, recv):
    b, u, c = place()
    greet(ring_greetings(u, c, nu))
    wires = Wires(send, recv)
    mine = c * nu + u
    half = part.shape[1] // 2

    def emit(span, total):
        residual = img_ref[span].astype(F32) + mod_ref[2:3] * total
        res_ref[span] = residual
        feed[mine, span] = normalized(residual, mod_ref[7:8], mod_ref[8:9]).astype(BF16)

    ring_sum(wires, part, relay, staged, inbox, u, nu, emit)
    ring_share(
        wires,
        [lambda s: feed.at[s, pl.ds(0, half)]],
        [lambda s: feed.at[s, pl.ds(half, half)]],
        u,
        c,
        nu,
    )
    all_ref[...] = feed[...]
    wires.drain()


def middle(mesh, part, img, mod):
    nu = mesh.shape["ulysses"]
    rows, depth = img.shape
    vm = pl.BlockSpec(memory_space=VMEM)
    return pl.pallas_call(
        functools.partial(middle_kernel, nu),
        out_shape=(
            jax.ShapeDtypeStruct((2 * nu, rows, depth), BF16),
            jax.ShapeDtypeStruct((rows, depth), F32),
        ),
        in_specs=[vm, vm, vm],
        out_specs=(vm, vm),
        scratch_shapes=[
            VMEM((2, rows // 2, depth), BF16),
            VMEM((2, rows // 2, depth), BF16),
            VMEM((2, rows, depth), BF16),
            VMEM((2 * nu, rows, depth), BF16),
            pltpu.SemaphoreType.DMA((32,)),
            pltpu.SemaphoreType.DMA((32,)),
        ],
        compiler_params=pltpu.CompilerParams(
            collective_id=4, has_side_effects=True, vmem_limit_bytes=VMEM_LIMIT
        ),
        name="middle",
    )(part, img, mod)


def last_kernel(
    nu, part, res_ref, mod_ref, fw_ref, out_ref, cross, summed, relay, staged, inbox, final, noise, send, recv
):
    b, u, c = place()
    greet(ring_greetings(u, c, nu))
    wires = Wires(send, recv)
    other = 1 - c
    right, left, opposite = (lax.rem(u + 1, nu), lax.rem(u + nu - 1, nu), lax.rem(u + 2, nu))
    order = (opposite, right, left, u)
    numbers = [wires.send(part.at[other, k], cross.at[k], cfg=other) for k in order]
    for number, k in zip(numbers, order):
        wires.arrive(number, cross.at[k], cfg=other)

        @pl.loop(0, part.shape[2], step=16)
        def _(at):
            span = pl.ds(pl.multiple_of(at, 16), 16)
            summed[k, span] = (part[c, k, span].astype(F32) + cross[k, span].astype(F32)).astype(BF16)

    def emit(span, total):
        second = res_ref[span] + mod_ref[9:10] * total
        final[span] = normalized(second, mod_ref[6:7], mod_ref[5:6]).astype(BF16)

    ring_sum(wires, summed, relay, staged, inbox, u, nu, emit)
    noise[c] = lax.dot_general(
        final[...], fw_ref[...], (((1,), (1,)), ((), ())), preferred_element_type=F32
    )
    swap = wires.send(noise.at[c], noise.at[c], cfg=other)
    wires.arrive(swap, noise.at[other], cfg=other)
    out_ref[...] = noise[1] + GUIDANCE * (noise[0] - noise[1])
    wires.drain()


def last(mesh, part, residual, mod, final_weight_t):
    nu = mesh.shape["ulysses"]
    rows, depth = residual.shape
    vm = pl.BlockSpec(memory_space=VMEM)
    return pl.pallas_call(
        functools.partial(last_kernel, nu),
        out_shape=jax.ShapeDtypeStruct((rows, 128), F32),
        in_specs=[vm, vm, vm, vm],
        out_specs=vm,
        scratch_shapes=[
            VMEM((nu, rows, depth), BF16),
            VMEM((nu, rows, depth), BF16),
            VMEM((2, rows // 2, depth), BF16),
            VMEM((2, rows // 2, depth), BF16),
            VMEM((2, rows, depth), BF16),
            VMEM((rows, depth), BF16),
            VMEM((2, rows, 128), F32),
            pltpu.SemaphoreType.DMA((16,)),
            pltpu.SemaphoreType.DMA((16,)),
        ],
        compiler_params=pltpu.CompilerParams(
            collective_id=5, has_side_effects=True, vmem_limit_bytes=VMEM_LIMIT
        ),
        name="last",
    )(part, residual, mod, final_weight_t)


def body(
    mesh,
    img_tokens,
    text_tokens,
    text_lengths,
    timestep,
    pooled,
    time_weight,
    time_second,
    mod_weight,
    proj_weight,
    out_weight,
    expand_weight,
    reduce_weight,
    qk_gain,
    final_weight,
):
    depth = img_tokens.shape[3]
    nb, nu = (mesh.shape["blk"], mesh.shape["ulysses"])
    image = img_tokens[0, 0]
    text = text_tokens[0, 0]
    rows, text_rows = (image.shape[0], text.shape[0])
    branch = lax.axis_index("cfg")
    expand_full = lax.all_gather(expand_weight, "blk", axis=0, tiled=True)
    reduce_full_t = lax.all_gather(reduce_weight.T, "blk", axis=0, tiled=True)

    sinusoid_rows = sinusoid(timestep, time_weight.shape[0]).astype(BF16)
    time_hidden = jax.nn.silu(
        jnp.dot(sinusoid_rows, time_weight, preferred_element_type=F32)
    ).astype(BF16)
    time_part = jnp.dot(time_hidden, time_second, preferred_element_type=F32)
    share = time_part.shape[1]
    row = jnp.concatenate([time_part, text_lengths.astype(F32)], axis=1)
    row = jnp.pad(row, ((0, 0), (0, 127 - share)))[None]
    times = spread(mesh, row, False, 0)
    time_embed = times[:, :, 0, :share].reshape(1, depth)
    lengths = times[0, 0:2, 0, share]
    acted = jax.nn.silu(time_embed + pooled[:, 0]).astype(BF16)
    mod_part = jnp.dot(acted, mod_weight, preferred_element_type=F32)
    columns = mod_part.shape[1]
    mod_rows = jnp.pad(mod_part, ((0, 0), (0, 256 - columns)))[:, None]
    mod = spread(mesh, mod_rows, True, 1)[:, :, 0, :columns].reshape(10, depth)

    position = jnp.arange(nb * 32, dtype=jnp.int32)
    within = position % 8
    slot = (position // 32) * (nu * text_rows) + (position % 32) // 8 * text_rows + within
    allowed = (within < text_rows)[None] & (slot[None].astype(F32) < lengths[:, None])
    bias = jnp.where(allowed, 0.0, NEG_FILL).astype(F32)[:, None]

    heads = proj_weight.shape[2] // qk_gain.shape[1]
    gain = jnp.tile(qk_gain, (1, heads))
    unit_rows = project(mesh, image, text, mod, gain, proj_weight)
    part = attention(mesh, unit_rows, bias, out_weight, rows)
    feed_all, residual = middle(mesh, part, image, mod)
    pre_active = jnp.dot(
        feed_all.reshape(-1, depth), expand_full, preferred_element_type=F32
    )
    feed_hidden = jax.nn.gelu(pre_active, approximate=True).astype(BF16)
    feed_part = lax.dot_general(
        feed_hidden, reduce_full_t, (((1,), (1,)), ((), ())), preferred_element_type=F32
    ).astype(BF16)
    final_t = jnp.pad(final_weight.T, ((0, 128 - final_weight.shape[1]), (0, 0)))
    guided = last(mesh, feed_part.reshape(2, nu, rows, depth), residual, mod, final_t)
    channels = final_weight.shape[1] // 4
    own = lax.dynamic_slice_in_dim(guided, branch * 2 * channels, 2 * channels, 1)
    own = own.reshape(rows, 2, channels).transpose(2, 0, 1)
    return own.reshape(1, channels, 1, 2 * rows)


def solution(mesh):
    in_specs = (
        P("cfg", "groups", ("blk", "ulysses"), None),
        P("cfg", "groups", ("blk", "ulysses"), None),
        P("cfg", "groups"),
        P("groups"),
        P(None, "groups", None),
        P(),
        P(None, ("blk", "ulysses", "cfg")),
        P(None, ("blk", "ulysses", "cfg")),
        P(None, None, ("ulysses", "cfg")),
        P(("ulysses", "cfg"), None),
        P("blk", ("ulysses", "cfg")),
        P(("ulysses", "cfg"), "blk"),
        P(),
        P(),
    )
    out_specs = P("groups", None, ("blk", "ulysses", "cfg"), None)
    return jax.shard_map(
        functools.partial(body, mesh), mesh=mesh, in_specs=in_specs, out_specs=out_specs, check_vma=False
    )
```
